32 devices in a mesh: data: 4 (over x, y), tp: 8 (over z, core).
Axes of the slice: x: 2, y: 2, z: 4, core: 2. Of those that a mesh axis runs over, the one named last changes fastest.
Arguments:
- x: bfloat16 [16384, 14336], P('data', 'tp'), parts along dimension 0
- w: bfloat16 [14336, 3584], P('tp')
- r: bfloat16 [16384, 3584], P('data'), parts along dimension 0
- g: bfloat16 [3584], replicated
Outputs:
- output: bfloat16 [16384, 3584], P('data'), parts along dimension 0
There are 4 independent parts. The reference program is written for one: setup_inputs(seed, part) draws one part's arguments, and reference() takes and returns one part's arrays. A program takes and returns all parts, laid end to end along the dimension named above; an argument that names none is the same for every part.
All inputs are finite; a program needn't handle non-finite values.
Results may differ from the reference program's by a relative error of at most 0.0108131.
Values are sent between devices in bfloat16 or wider.
A program may use at most 1 GiB of HBM per device.

```python
import jax
import jax.numpy as jnp
from jax import lax

T = 4096
H = 3584
F = 14336
EPS = 1e-6


def setup_inputs(seed: int = 0, part: int = 0) -> dict:
    kp = jax.random.fold_in(jax.random.key(seed), part)
    kx, kr = jax.random.split(kp)
    kw, kg = jax.random.split(jax.random.key(seed + 1))
    x = jax.random.normal(kx, (T, F), jnp.float32).astype(jnp.bfloat16)
    w = (jax.random.normal(kw, (F, H), jnp.float32) * (F ** -0.5)).astype(jnp.bfloat16)
    r = jax.random.normal(kr, (T, H), jnp.float32).astype(jnp.bfloat16)
    g = jax.random.uniform(kg, (H,), jnp.float32, 0.5, 1.5).astype(jnp.bfloat16)
    return {"x": x, "w": w, "r": r, "g": g}


def reference(x, w, r, g):
    y = jnp.dot(x, w, preferred_element_type=jnp.float32).astype(jnp.bfloat16)
    a = r.astype(jnp.float32) + y.astype(jnp.float32)
    ms = jnp.mean(a * a, axis=-1, keepdims=True)
    z = a * lax.rsqrt(ms + EPS) * g.astype(jnp.float32)
    return z.astype(jnp.bfloat16)
```

```python
import functools

import jax
import jax.numpy as jnp
from jax import lax
from jax.experimental import pallas as pl
from jax.experimental.pallas import tpu as pltpu
from jax.sharding import PartitionSpec as P

EPS = 1e-6
BF = jnp.bfloat16
F32 = jnp.float32

C = 32
Q = 4
NT = 512
PIECE = 512
D = 12
NS = 4
NL = 2
LAGS = (6, 0, 6, 10)


def kernel(
    x_hbm, w_hbm, r_hbm, g_ref, z_ref,
    w_v, x_v, own_v, stage_v, land_v, a_v, b_v, s_v, r_v, f_v,
    w_sem, x_sem, r_sem, dsend, drecv, ssend, arecv, brecv, zrecv, zs_up, zs_dn, zs_d, zdrecv, credit,
):
    rows = z_ref.shape[0]
    half = rows // 2
    hid = z_ref.shape[1]
    mb = C * Q
    nb = half // mb
    nk = half // C
    nt = hid // NT

    me = lax.axis_index("tp")
    core = lax.rem(me, 2)
    zz = lax.div(me, 2)
    p = jnp.where(core == 0, zz, 3 - zz)
    step = 2 - 4 * core
    up, down = me - step, me + step
    partner = me + 1 - 2 * core
    mine = core * half
    other = half - mine
    lag = jnp.where(p == 3, LAGS[3], jnp.where(p == 2, LAGS[2], LAGS[0]))

    def remote(src, dst, send, recv, dev):
        return pltpu.make_async_remote_copy(
            src_ref=src, dst_ref=dst, send_sem=send, recv_sem=recv,
            device_id={"tp": dev}, device_id_type=pl.DeviceIdType.MESH,
        )

    def w_copy(j):
        cols = pl.ds(pl.multiple_of(j * NT, NT), NT)
        return pltpu.make_async_copy(w_hbm.at[:, cols], w_v.at[:, cols], w_sem.at[j])

    def x_copies(b, slot):
        return [
            pltpu.make_async_copy(
                x_hbm.at[pl.ds(pl.multiple_of(base + b * mb, mb), mb)],
                x_v.at[slot, pl.ds(i * mb, mb)],
                x_sem.at[slot, i],
            )
            for i, base in enumerate((mine, other))
        ]

    def r_copy(k):
        return pltpu.make_async_copy(
            r_hbm.at[pl.ds(pl.multiple_of(mine + k * C, C), C)], r_v.at[lax.rem(k, 2)], r_sem.at[lax.rem(k, 2)]
        )

    def stage_copy(b):
        return remote(
            stage_v.at[lax.rem(b, 2)], land_v.at[lax.rem(b, NL)],
            dsend.at[lax.rem(b, 2)], drecv.at[lax.rem(b, NL)], partner,
        )

    def s_copy(k, dst, recv, dev):
        return remote(s_v.at[lax.rem(k, NS)], dst.at[lax.rem(k, D)], ssend.at[lax.rem(k, NS)], recv.at[lax.rem(k, D)], dev)

    def z_rows(k):
        return z_ref.at[pl.ds(pl.multiple_of(mine + k * C, C), C)]

    def z_copy(k, send, recv, dev):
        return remote(z_rows(k), z_rows(k), send, recv, dev)

    def matmul(b):
        slot = lax.rem(b, 2)
        for copy in x_copies(b, slot):
            copy.wait()

        @pl.when(b + 1 < nb)
        def _():
            for copy in x_copies(b + 1, 1 - slot):
                copy.start()

        @pl.when(b >= 2)
        def _():
            stage_copy(b - 2).wait_send()

        def tile(j, carry):
            @pl.when(b == 0)
            def _():
                w_copy(j).wait()

            cols = pl.ds(pl.multiple_of(j * NT, NT), NT)
            acc = jnp.dot(x_v[slot], w_v[:, cols], preferred_element_type=F32)
            own_v[slot, :, cols] = acc[:mb].astype(BF)
            stage_v[slot, :, cols] = acc[mb:].astype(BF)
            return carry

        lax.fori_loop(0, nt, tile, 0)

        @pl.when(b >= NL)
        def _():
            pl.semaphore_wait(credit, 1)

        stage_copy(b).start()

    def send_sum(k, add, dst, recv, dev):
        b, q = lax.div(k, Q), lax.rem(k, Q)
        slot, here, ss = lax.rem(b, 2), pl.ds(pl.multiple_of(q * C, C), C), lax.rem(k, NS)

        @pl.when(k >= NS)
        def _():
            s_copy(k - NS, dst, recv, dev).wait_send()

        for j in range(hid // PIECE):
            cols = pl.ds(j * PIECE, PIECE)
            t = own_v[slot, here, cols].astype(F32) + land_v[lax.rem(b, NL), here, cols].astype(F32)
            if add is not None:
                t += add[lax.rem(k, D), :, cols].astype(F32)
            s_v[ss, :, cols] = t.astype(BF)
        s_copy(k, dst, recv, dev).start()

    def root(k):
        b, q = lax.div(k, Q), lax.rem(k, Q)
        slot, here, ks = lax.rem(b, 2), pl.ds(pl.multiple_of(q * C, C), C), lax.rem(k, D)
        out = pl.ds(pl.multiple_of(mine + k * C, C), C)

        @pl.when(k + 1 < nk)
        def _():
            r_copy(k + 1).start()

        r_copy(k).wait()
        s_copy(k, b_v, brecv, me).wait_recv()
        s_copy(k, a_v, arecv, me).wait_recv()
        ss = jnp.zeros((C, PIECE), F32)
        for j in range(hid // PIECE):
            cols = pl.ds(j * PIECE, PIECE)
            t = own_v[slot, here, cols].astype(F32) + land_v[lax.rem(b, NL), here, cols].astype(F32)
            t += b_v[ks, :, cols].astype(F32)
            t += a_v[ks, :, cols].astype(F32)
            a = r_v[lax.rem(k, 2), :, cols].astype(F32) + t.astype(BF).astype(F32)
            f_v[:, cols] = a
            ss += a * a
        scale = lax.rsqrt(jnp.sum(ss, axis=-1, keepdims=True) * (1.0 / hid) + EPS)
        for j in range(hid // PIECE):
            cols = pl.ds(j * PIECE, PIECE)
            z_ref[out, cols] = (f_v[:, cols] * scale * g_ref[:, cols].astype(F32)).astype(BF)
        z_copy(k, zs_up, zrecv.at[k], up).start()
        z_copy(k, zs_dn, zrecv.at[k], down).start()
        z_copy(k, zs_d, zdrecv, partner).start()

    def pass_on(j):
        @pl.when((p != 1) & (j >= 0))
        def _():
            z_copy(j, zs_d, zrecv.at[j], partner).wait_recv()

            @pl.when(p == 2)
            def _():
                z_copy(j, zs_dn, zrecv.at[j], down).start()

            z_copy(j, zs_d, zdrecv, partner).start()

    def chunk(k, carry):
        b, q = lax.div(k, Q), lax.rem(k, Q)

        @pl.when(q == 0)
        def _():
            stage_copy(b).wait_recv()

        @pl.when(p == 0)
        def _():
            send_sum(k, None, b_v, brecv, down)

        @pl.when(p == 3)
        def _():
            send_sum(k, None, a_v, arecv, up)

        @pl.when(p == 2)
        def _():
            s_copy(k, a_v, arecv, me).wait_recv()
            send_sum(k, a_v, a_v, arecv, up)

        @pl.when(p == 1)
        def _():
            root(k)

        @pl.when((q == Q - 1) & (b < nb - NL))
        def _():
            pl.semaphore_signal(credit, inc=1, device_id={"tp": partner}, device_id_type=pl.DeviceIdType.MESH)

        pass_on(k - lag)

        @pl.when((q == 1) & (b + 1 < nb))
        def _():
            matmul(b + 1)

        return carry

    def drain(k, carry):
        @pl.when(k - lag < nk)
        def _():
            pass_on(k - lag)

        return carry

    for copy in x_copies(0, 0):
        copy.start()

    def w_start(j, carry):
        w_copy(j).start()
        return carry

    lax.fori_loop(0, nt, w_start, 0)

    @pl.when(p == 1)
    def _():
        r_copy(0).start()

    matmul(0)
    lax.fori_loop(0, nk, chunk, 0)
    lax.fori_loop(nk, nk + max(LAGS), drain, 0)

    for b in range(nb - 2, nb):
        stage_copy(b).wait_send()

    @pl.when(p != 1)
    def _():
        for k in range(nk - NS, nk):
            s_copy(k, a_v, arecv, me).wait_send()

    def whole(base, send, recv):
        ref = z_ref.at[pl.ds(pl.multiple_of(base, half), half)]
        return remote(ref, ref, send, recv, partner)

    @pl.when(p == 1)
    def _():
        whole(mine, zs_up, zdrecv).wait_send()

    @pl.when((p == 1) | (p == 2))
    def _():
        whole(mine, zs_dn, zdrecv).wait_send()

    whole(mine, zs_d, zdrecv).wait_send()
    whole(other, zs_d, zdrecv).wait_recv()


def solution(mesh):
    assert mesh.shape["tp"] == 8

    def local(x, w, r, g):
        rows, depth = x.shape
        hid = w.shape[1]
        half = rows // 2
        mb = C * Q
        nk = half // C
        anyspace = pl.BlockSpec(memory_space=pl.ANY)
        vmem = pl.BlockSpec(memory_space=pltpu.VMEM)
        dma = pltpu.SemaphoreType.DMA
        return pl.pallas_call(
            kernel,
            out_shape=jax.ShapeDtypeStruct((rows, hid), BF),
            in_specs=[anyspace, anyspace, anyspace, vmem],
            out_specs=vmem,
            scratch_shapes=[
                pltpu.VMEM((depth, hid), BF),
                pltpu.VMEM((2, 2 * mb, depth), BF),
                pltpu.VMEM((2, mb, hid), BF),
                pltpu.VMEM((2, mb, hid), BF),
                pltpu.VMEM((NL, mb, hid), BF),
                pltpu.VMEM((D, C, hid), BF),
                pltpu.VMEM((D, C, hid), BF),
                pltpu.VMEM((NS, C, hid), BF),
                pltpu.VMEM((2, C, hid), BF),
                pltpu.VMEM((C, hid), F32),
                dma((hid // NT,)),
                dma((2, 2)),
                dma((2,)),
                dma((2,)),
                dma((NL,)),
                dma((NS,)),
                dma((D,)),
                dma((D,)),
                dma((nk,)),
                dma,
                dma,
                dma,
                dma,
                pltpu.SemaphoreType.REGULAR,
            ],
            compiler_params=pltpu.CompilerParams(has_side_effects=True, vmem_limit_bytes=67043328),
            cost_estimate=pl.CostEstimate(
                flops=2 * rows * depth * hid,
                bytes_accessed=2 * (rows * depth + depth * hid + 2 * rows * hid),
                transcendentals=rows,
            ),
        )(x, w, r, g.reshape(1, hid))

    return jax.shard_map(
        local,
        mesh=mesh,
        in_specs=(P("data", "tp"), P("tp", None), P("data", None), P(None)),
        out_specs=P("data", None),
        check_vma=False,
    )
```

```python
import functools

import jax
import jax.numpy as jnp
from jax import lax
from jax.experimental import pallas as pl
from jax.experimental.pallas import tpu as pltpu
from jax.sharding import PartitionSpec as P

EPS = 1e-6
BF = jnp.bfloat16
F32 = jnp.float32

C = 16
Q = 8
NT = 512
PIECE = 512
D = 20
NS = 8
NL = 3
LAGS = (12, 0, 4, 14)
TQ = 2
OUT = 8


def kernel(
    x_hbm, w_hbm, r_hbm, g_hbm, z_ref,
    w_v, x_v, own_v, stage_v, land_v, a_v, b_v, s_v, r_v, f_v, g_v, g_raw,
    w_sem, x_sem, r_sem, dsend, drecv, ssend, arecv, brecv, zrecv, zs_up, zs_dn, zs_d, zdrecv, g_sem, credit,
):
    rows = z_ref.shape[0]
    half = rows // 2
    hid = z_ref.shape[1]
    mb = C * Q
    nb = half // mb
    nk = half // C
    nt = hid // NT

    me = lax.axis_index("tp")
    core = lax.rem(me, 2)
    zz = lax.div(me, 2)
    p = jnp.where(core == 0, zz, 3 - zz)
    step = 2 - 4 * core
    up, down = me - step, me + step
    partner = me + 1 - 2 * core
    mine = core * half
    other = half - mine
    leaf = (p == 0) | (p == 3)
    lag = jnp.where(p == 3, LAGS[3], jnp.where(p == 2, LAGS[2], LAGS[0]))

    def remote(src, dst, send, recv, dev):
        return pltpu.make_async_remote_copy(
            src_ref=src, dst_ref=dst, send_sem=send, recv_sem=recv,
            device_id={"tp": dev}, device_id_type=pl.DeviceIdType.MESH,
        )

    def w_copy(j):
        cols = pl.ds(pl.multiple_of(j * NT, NT), NT)
        return pltpu.make_async_copy(w_hbm.at[:, cols], w_v.at[:, cols], w_sem.at[j])

    def x_copies(b, slot):
        return [
            pltpu.make_async_copy(
                x_hbm.at[pl.ds(pl.multiple_of(base + b * mb, mb), mb)],
                x_v.at[slot, pl.ds(i * mb, mb)],
                x_sem.at[slot, i],
            )
            for i, base in enumerate((mine, other))
        ]

    def r_copy(k):
        return pltpu.make_async_copy(
            r_hbm.at[pl.ds(pl.multiple_of(mine + k * C, C), C)], r_v.at[lax.rem(k, 2)], r_sem.at[lax.rem(k, 2)]
        )

    def stage_copy(b, cols=slice(None)):
        slot, there = lax.rem(b, 2), lax.rem(b, NL)
        return remote(stage_v.at[slot, :, cols], land_v.at[there, :, cols], dsend.at[slot], drecv.at[there], partner)

    def s_copy(k, dst, recv, dev):
        return remote(s_v.at[lax.rem(k, NS)], dst.at[lax.rem(k, D)], ssend.at[lax.rem(k, NS)], recv.at[lax.rem(k, D)], dev)

    def z_rows(k):
        return z_ref.at[pl.ds(pl.multiple_of(mine + k * C, C), C)]

    def z_copy(k, send, recv, dev):
        return remote(z_rows(k), z_rows(k), send, recv, dev)

    def open_block(b):
        slot = lax.rem(b, 2)
        for copy in x_copies(b, slot):
            copy.wait()

        @pl.when(b + 1 < nb)
        def _():
            for copy in x_copies(b + 1, 1 - slot):
                copy.start()

        @pl.when(b >= 2)
        def _():
            stage_copy(b - 2).wait_send()

        @pl.when(b >= NL)
        def _():
            pl.semaphore_wait(credit, 1)

    def tile(b, j, ready=None):
        slot = lax.rem(b, 2)
        cols = pl.ds(pl.multiple_of(j * NT, NT), NT)
        acc = jnp.dot(x_v[slot], w_v[:, cols], preferred_element_type=F32)
        stage_v[slot, :, cols] = acc[mb:].astype(BF)
        own_v[slot, :, cols] = acc[:mb].astype(BF)
        if ready is not None:
            ready()
        stage_copy(b, cols).start()

    def tiles(b, q):
        @pl.when((b < nb) & (q == 0))
        def _():
            open_block(b)

        for i in range(TQ):

            @pl.when((b < nb) & (q * TQ + i < nt))
            def _():
                tile(b, q * TQ + i)

    def send_sum(k, add, dst, recv, dev):
        b, q = lax.div(k, Q), lax.rem(k, Q)
        slot, here, ss = lax.rem(b, 2), pl.ds(pl.multiple_of(q * C, C), C), lax.rem(k, NS)

        @pl.when(k >= NS)
        def _():
            s_copy(k - NS, dst, recv, dev).wait_send()

        for j in range(hid // PIECE):
            cols = pl.ds(j * PIECE, PIECE)
            t = own_v[slot, here, cols].astype(F32) + land_v[lax.rem(b, NL), here, cols].astype(F32)
            if add is not None:
                t += add[lax.rem(k, D), :, cols].astype(F32)
            s_v[ss, :, cols] = t.astype(BF)
        s_copy(k, dst, recv, dev).start()

    def root(k):
        b, q = lax.div(k, Q), lax.rem(k, Q)
        slot, here, ks = lax.rem(b, 2), pl.ds(pl.multiple_of(q * C, C), C), lax.rem(k, D)
        out = pl.ds(pl.multiple_of(mine + k * C, C), C)

        @pl.when(k + 1 < nk)
        def _():
            r_copy(k + 1).start()

        r_copy(k).wait()
        s_copy(k, b_v, brecv, me).wait_recv()
        s_copy(k, a_v, arecv, me).wait_recv()
        ss = jnp.zeros((C, PIECE), F32)
        for j in range(hid // PIECE):
            cols = pl.ds(j * PIECE, PIECE)
            t = own_v[slot, here, cols].astype(F32) + land_v[lax.rem(b, NL), here, cols].astype(F32)
            t += b_v[ks, :, cols].astype(F32)
            t += a_v[ks, :, cols].astype(F32)
            a = r_v[lax.rem(k, 2), :, cols].astype(F32) + t.astype(BF).astype(F32)
            f_v[:, cols] = a
            ss += a * a
        scale = lax.rsqrt(jnp.sum(ss, axis=-1, keepdims=True) * (1.0 / hid) + EPS)
        for j in range(hid // PIECE):
            cols = pl.ds(j * PIECE, PIECE)
            z_ref[out, cols] = (f_v[:, cols] * scale * g_v[:, cols]).astype(BF)
        z_copy(k, zs_up, zrecv.at[k], up).start()
        z_copy(k, zs_dn, zrecv.at[k], down).start()
        z_copy(k, zs_d, zdrecv, partner).start()

    def pass_on(j):
        @pl.when((p != 1) & (j >= 0))
        def _():
            z_copy(j, zs_d, zrecv.at[j], partner).wait_recv()

            @pl.when(p == 2)
            def _():
                z_copy(j, zs_dn, zrecv.at[j], down).start()

            z_copy(j, zs_d, zdrecv, partner).start()

    def chunk(k, carry):
        b, q = lax.div(k, Q), lax.rem(k, Q)

        @pl.when(jnp.logical_not(leaf))
        def _():
            tiles(b + 1, q)

        @pl.when(q == 0)
        def _():
            stage_copy(b).wait_recv()

        @pl.when(p == 0)
        def _():
            send_sum(k, None, b_v, brecv, down)

        @pl.when(p == 3)
        def _():
            send_sum(k, None, a_v, arecv, up)

        @pl.when(p == 2)
        def _():
            s_copy(k, a_v, arecv, me).wait_recv()
            send_sum(k, a_v, a_v, arecv, up)

        @pl.when(p == 1)
        def _():
            root(k)

        @pl.when((q == Q - 1) & (b < nb - NL))
        def _():
            pl.semaphore_signal(credit, inc=1, device_id={"tp": partner}, device_id_type=pl.DeviceIdType.MESH)

        pass_on(k - lag)

        @pl.when(leaf)
        def _():
            tiles(b + 1, q)

        return carry

    def drain(k, carry):
        @pl.when(k - lag < nk)
        def _():
            pass_on(k - lag)

        return carry

    for copy in x_copies(0, 0):
        copy.start()

    def w_start(j, carry):
        w_copy(j).start()
        return carry

    lax.fori_loop(0, nt, w_start, 0)
    g_copy = pltpu.make_async_copy(g_hbm, g_raw, g_sem)
    g_copy.start()

    @pl.when(p == 1)
    def _():
        r_copy(0).start()

    barrier = pltpu.get_barrier_semaphore()

    def greet(dev):
        pl.semaphore_signal(barrier, inc=1, device_id={"tp": dev}, device_id_type=pl.DeviceIdType.MESH)

    greet(partner)

    @pl.when(p != 0)
    def _():
        greet(up)

    @pl.when(p != 3)
    def _():
        greet(down)

    open_block(0)

    def met():
        pl.semaphore_wait(barrier, jnp.where(leaf, 2, 3))

    w_copy(0).wait()
    tile(0, 0, met)

    def first(j, carry):
        w_copy(j).wait()
        tile(0, j)
        return carry

    lax.fori_loop(1, nt, first, 0)
    g_copy.wait()
    for j in range(hid // PIECE):
        cols = pl.ds(j * PIECE, PIECE)
        g_v[:, cols] = g_raw[cols].astype(F32).reshape(1, PIECE)
    lax.fori_loop(0, nk, chunk, 0)
    lax.fori_loop(nk, nk + max(LAGS), drain, 0)

    for b in range(nb - 2, nb):
        stage_copy(b).wait_send()

    @pl.when(p != 1)
    def _():
        for k in range(nk - NS, nk):
            s_copy(k, a_v, arecv, me).wait_send()

    def whole(base, send, recv):
        ref = z_ref.at[pl.ds(pl.multiple_of(base, half), half)]
        return remote(ref, ref, send, recv, partner)

    @pl.when(p == 1)
    def _():
        whole(mine, zs_up, zdrecv).wait_send()

    @pl.when((p == 1) | (p == 2))
    def _():
        whole(mine, zs_dn, zdrecv).wait_send()

    whole(mine, zs_d, zdrecv).wait_send()
    whole(other, zs_d, zdrecv).wait_recv()


def put(n, z_ref, out_ref, sem):
    rows = z_ref.shape[0] // n
    copies = [
        pltpu.make_async_copy(z_ref.at[pl.ds(i * rows, rows)], out_ref.at[pl.ds(i * rows, rows)], sem.at[i])
        for i in range(n)
    ]
    for copy in copies:
        copy.start()
    for copy in copies:
        copy.wait()


def solution(mesh):
    assert mesh.shape["tp"] == 8

    def local(x, w, r, g):
        rows, depth = x.shape
        hid = w.shape[1]
        half = rows // 2
        mb = C * Q
        nk = half // C
        anyspace = pl.BlockSpec(memory_space=pl.ANY)
        vmem = pl.BlockSpec(memory_space=pltpu.VMEM)
        dma = pltpu.SemaphoreType.DMA
        z = pl.pallas_call(
            kernel,
            out_shape=pltpu.VMEM((rows, hid), BF),
            in_specs=[anyspace, anyspace, anyspace, anyspace],
            out_specs=vmem,
            scratch_shapes=[
                pltpu.VMEM((depth, hid), BF),
                pltpu.VMEM((2, 2 * mb, depth), BF),
                pltpu.VMEM((2, mb, hid), BF),
                pltpu.VMEM((2, mb, hid), BF),
                pltpu.VMEM((NL, mb, hid), BF),
                pltpu.VMEM((D, C, hid), BF),
                pltpu.VMEM((D, C, hid), BF),
                pltpu.VMEM((NS, C, hid), BF),
                pltpu.VMEM((2, C, hid), BF),
                pltpu.VMEM((C, hid), F32),
                pltpu.VMEM((1, hid), F32),
                pltpu.VMEM((hid,), BF),
                dma((hid // NT,)),
                dma((2, 2)),
                dma((2,)),
                dma((2,)),
                dma((NL,)),
                dma((NS,)),
                dma((D,)),
                dma((D,)),
                dma((nk,)),
                dma,
                dma,
                dma,
                dma,
                dma,
                pltpu.SemaphoreType.REGULAR,
            ],
            compiler_params=pltpu.CompilerParams(has_side_effects=True, collective_id=0, vmem_limit_bytes=34 * 2**20),
            cost_estimate=pl.CostEstimate(
                flops=2 * rows * depth * hid,
                bytes_accessed=2 * (rows * depth + depth * hid + 2 * rows * hid),
                transcendentals=rows,
            ),
        )(x, w, r, g)
        return pl.pallas_call(
            functools.partial(put, OUT),
            out_shape=jax.ShapeDtypeStruct((rows, hid), BF),
            in_specs=[vmem],
            out_specs=anyspace,
            scratch_shapes=[dma((OUT,))],
            compiler_params=pltpu.CompilerParams(vmem_limit_bytes=2**20),
        )(z)

    return jax.shard_map(
        local,
        mesh=mesh,
        in_specs=(P("data", "tp"), P("tp", None), P("data", None), P(None)),
        out_specs=P("data", None),
        check_vma=False,
    )
```
